256 devices in a mesh: img: 16 (over y, x), row: 16 (over z, core).
Axes of the slice: x: 4, y: 4, z: 8, core: 2. Of those that a mesh axis runs over, the one named last changes fastest.
Arguments:
- latent: bfloat16 [1024, 128, 512], P(('img', 'row')), parts along dimension 0, may hold values from -8 to 8
- attn_gain: float32 [512], replicated, may hold values from 0.5 to 1.5
- attn_shift: float32 [512], replicated, may hold values from -3 to 3
- w_query: bfloat16 [512, 512], replicated, may hold values from -2 to 2
- w_key: bfloat16 [512, 512], replicated, may hold values from -2 to 2
- w_value: bfloat16 [512, 512], replicated, may hold values from -0.25 to 0.25
- w_out: bfloat16 [512, 512], replicated, may hold values from -0.25 to 0.25
- conv_gain: float32 [512], replicated, may hold values from 0.5 to 1.5
- conv_shift: float32 [512], replicated, may hold values from -3 to 3
- w_conv: bfloat16 [3, 3, 512, 512], replicated, may hold values from -0.09375 to 0.09375
- conv_bias: float32 [512], replicated, may hold values from -3 to 3
Outputs:
- encoded: bfloat16 [1024, 128, 512], P(('img', 'row')), parts along dimension 0
The draws below stay inside these ranges and needn't reach their ends.
There are 16 independent parts, one for each index of `img`. The reference program is written for one: setup_inputs(seed, part) draws one part's arguments, and reference() takes and returns one part's arrays. A program takes and returns all parts, laid end to end along the dimension named above; an argument that names none is the same for every part. Nothing has to cross between parts.
All inputs are finite; a program needn't handle non-finite values.
Results may differ from the reference program's by a relative error of at most 0.011.
Values may be sent and summed in bfloat16 or wider, within the bound.
No kernel may reach another device: no remote copies, remote signals or barrier semaphores. Data moves between devices by JAX's collectives and lax.ppermute only.
A program may use at most 128 MiB of HBM per device.

```python
import jax
import jax.numpy as jnp
from jax import lax

C = 512
GROUPS = 32
W = 128
H = 64


def shared_gauss(key):
    return jnp.clip(jax.random.normal(jax.random.fold_in(key, 7), (C, C), jnp.float32), -3.0, 3.0)


def draw_latent(key, part):
    noise = jax.random.normal(jax.random.fold_in(key, 3), (H, W, C), jnp.float32)
    rows = (jnp.arange(H, dtype=jnp.float32) + 0.5) / H
    phase = jax.random.uniform(jax.random.fold_in(key, 13), (GROUPS,), jnp.float32, -jnp.pi, jnp.pi)
    amplitude = jax.random.uniform(jax.random.fold_in(key, 17), (C,), jnp.float32, 0.8, 1.6)
    wave = jnp.sin(2.0 * jnp.pi * rows[:, None] + phase[None, :])
    offset = jnp.repeat(wave, C // GROUPS, axis=1) * amplitude[None, :]
    result = noise + offset[:, None, :]
    return jnp.clip(result, -8.0, 8.0).astype(jnp.bfloat16)


def draw_w_query(key, part):
    return (shared_gauss(key) * (4.0 / jnp.sqrt(jnp.float32(C)))).astype(jnp.bfloat16)


def draw_w_key(key, part):
    fresh = jnp.clip(jax.random.normal(jax.random.fold_in(key, 11), (C, C), jnp.float32), -3.0, 3.0)
    result = fresh / jnp.sqrt(jnp.float32(C))
    return result.astype(jnp.bfloat16)


def scatter_about(stream_key, extent, scale, most, kind=jnp.bfloat16):
    return jnp.clip(scale * jax.random.normal(stream_key, extent, jnp.float32), -most, most).astype(kind)


def setup_inputs(seed: int = 0, part: int = 0) -> dict:
    key_list = jax.random.split(jax.random.key(seed), 12)
    part_splits = jax.random.split(jax.random.fold_in(key_list[11], part), 12)
    return {
        "latent": draw_latent(jax.random.fold_in(jax.random.fold_in(key_list[11], part), 71), part),
        "attn_gain": jnp.clip(1.0 + 0.1 * jax.random.normal(key_list[1], (C,), jnp.float32), 0.5, 1.5),
        "attn_shift": scatter_about(key_list[2], (C,), 0.5, 3.0, jnp.float32),
        "w_query": draw_w_query(jax.random.fold_in(key_list[11], 71), part),
        "w_key": draw_w_key(jax.random.fold_in(key_list[11], 71), part),
        "w_value": scatter_about(key_list[5], (C, C), C ** -0.5, 0.25),
        "w_out": scatter_about(key_list[6], (C, C), C ** -0.5, 0.25),
        "conv_gain": jnp.clip(1.0 + 0.1 * jax.random.normal(key_list[7], (C,), jnp.float32), 0.5, 1.5),
        "conv_shift": scatter_about(key_list[8], (C,), 0.5, 3.0, jnp.float32),
        "w_conv": scatter_about(key_list[9], (3, 3, C, C), (9 * C) ** -0.5, 0.09375),
        "conv_bias": scatter_about(key_list[10], (C,), 0.5, 3.0, jnp.float32),
    }


epsilon = 1e-06

def group_norm(field, gain, shift):
    grouped = field.astype(jnp.float32).reshape(field.shape[0], GROUPS, C // GROUPS)
    centre = lax.optimization_barrier(jnp.mean(grouped, axis=(0, 2)))
    offset = grouped - centre[None, :, None]
    spread = lax.optimization_barrier(jnp.mean(offset * offset, axis=(0, 2)))
    normed = offset * lax.rsqrt(spread + epsilon)[None, :, None]
    return normed.reshape(field.shape) * gain + shift

def reference(latent, attn_gain, attn_shift, w_query, w_key, w_value, w_out, conv_gain, conv_shift, w_conv, conv_bias):
    positions = latent.reshape(H * W, C)
    normed = group_norm(positions, attn_gain, attn_shift).astype(jnp.bfloat16)
    queries = jnp.dot(normed, w_query, preferred_element_type=jnp.float32).astype(jnp.bfloat16)
    key_rows = jnp.dot(normed, w_key, preferred_element_type=jnp.float32).astype(jnp.bfloat16)
    values = jnp.dot(normed, w_value, preferred_element_type=jnp.float32).astype(jnp.bfloat16)
    scaling = 1.0 / jnp.sqrt(jnp.float32(C))
    scores = jnp.einsum('qc,kc->qk', queries.astype(jnp.float32), key_rows.astype(jnp.float32)) * scaling
    rowmax = lax.optimization_barrier(jnp.max(scores, axis=1))
    expo = jnp.exp(scores - rowmax[:, None])
    denominator = lax.optimization_barrier(jnp.sum(expo, axis=1))
    probs = expo.astype(jnp.bfloat16)
    attended = (jnp.dot(probs, values, preferred_element_type=jnp.float32) / denominator[:, None]).astype(jnp.bfloat16)
    hidden = (positions.astype(jnp.float32) + jnp.dot(attended, w_out, preferred_element_type=jnp.float32)).astype(jnp.bfloat16)
    activated = jax.nn.silu(group_norm(hidden, conv_gain, conv_shift)).astype(jnp.bfloat16).reshape(H, W, C)
    padded = jnp.pad(activated, ((1, 1), (1, 1), (0, 0)))
    convolved = jnp.zeros((H * W, C), jnp.float32)
    for row_tap in range(3):
        for col_tap in range(3):
            window = padded[row_tap:row_tap + H, col_tap:col_tap + W].reshape(H * W, C)
            convolved = convolved + jnp.dot(window, w_conv[row_tap, col_tap], preferred_element_type=jnp.float32)
    encoded = hidden.astype(jnp.float32) + (convolved + conv_bias)
    return encoded.astype(jnp.bfloat16).reshape(H, W, C)
```

```python
import jax
import jax.numpy as jnp
from jax import lax
from jax.experimental import pallas as pl
from jax.experimental.pallas import tpu as pltpu
from jax.sharding import PartitionSpec as P

C = 512
GROUPS = 32
W = 128
LANES = 128
EPS = 1e-06
LOG2E = 1.4426950408889634
VMEM = pl.BlockSpec(memory_space=pltpu.VMEM)
SMEM = pl.BlockSpec(memory_space=pltpu.SMEM)
F32 = jnp.float32
BF16 = jnp.bfloat16
MIB = 1024 * 1024


def call(kernel, outs, specs, args, flops, vmem_mib=16, scratch=(), aliases=None):
    moved = sum(a.size * a.dtype.itemsize for a in args)
    return pl.pallas_call(
        kernel,
        out_shape=outs,
        in_specs=specs,
        out_specs=jax.tree.map(lambda _: VMEM, outs),
        scratch_shapes=list(scratch),
        input_output_aliases=aliases or {},
        cost_estimate=pl.CostEstimate(flops=flops, bytes_accessed=moved, transcendentals=0),
        compiler_params=pltpu.CompilerParams(vmem_limit_bytes=vmem_mib * MIB),
    )(*args)


def group_sum(v):
    lane = lax.broadcasted_iota(jnp.int32, v.shape, 1)
    for k in (1, 2, 4, 8):
        up = pltpu.roll(v, k, 1)
        down = pltpu.roll(v, C - k, 1)
        v = v + jnp.where((lane & k) != 0, up, down)
    return v


def write_stats(field, out_ref):
    rows = field.shape[0]
    share = C // GROUPS
    mean = group_sum(jnp.broadcast_to(jnp.sum(field, 0, keepdims=True), (8, C))) * (
        1.0 / (rows * share)
    )
    offset = field - mean[0:1]
    spread = group_sum(jnp.broadcast_to(jnp.sum(offset * offset, 0, keepdims=True), (8, C)))
    for i in range(C // LANES):
        cut = slice(i * LANES, (i + 1) * LANES)
        out_ref[i : i + 1, :] = mean[0:1, cut]
        out_ref[i + 4 : i + 5, :] = spread[0:1, cut]


def affine(stats, gain, shift, rows):
    count = stats.shape[0]
    local = rows * (C // GROUPS)
    means = stats[:, 0:4, :]
    mean = jnp.sum(means, 0) * (1.0 / count)
    offset = means - mean[None]
    total = jnp.sum(stats[:, 4:8, :], 0) + local * jnp.sum(offset * offset, 0)
    inverse = lax.rsqrt(total * (1.0 / (local * count)) + EPS)
    flat = lambda v: jnp.concatenate([v[i : i + 1] for i in range(4)], axis=1)
    scale = flat(inverse) * gain
    return scale, shift - flat(mean) * scale


def stats_kernel(x_ref, out_ref):
    write_stats(x_ref[...].astype(F32), out_ref)


def query_kernel(x_ref, stats_ref, gain_ref, shift_ref, wqk_ref, q_ref, coef_ref):
    scale, shift = affine(stats_ref[...], gain_ref[...], shift_ref[...], x_ref.shape[0])
    coef_ref[0:1, :] = scale
    coef_ref[1:2, :] = shift
    normed = (x_ref[...].astype(F32) * scale + shift).astype(BF16)
    q = jnp.dot(normed, wqk_ref[...], preferred_element_type=F32)
    q_ref[...] = (q * (scale * (LOG2E / C**0.5))).astype(BF16)


BLOCK = 256


def attend_kernel(first, last, own_ref, other_ref, ka_ref, kb_ref, *refs):
    if first:
        state, outs = None, refs
    else:
        state, outs = refs[:3], refs[3:]
    half = own_ref.shape[0]
    blocks = 2 * half // BLOCK
    keys = [ka_ref, kb_ref]

    def scores(i):
        src = own_ref if i * BLOCK < half else other_ref
        at = (i * BLOCK) % half
        q = src[at : at + BLOCK, :]
        return [
            lax.dot_general(q, k[...], (((1,), (1,)), ((), ())), preferred_element_type=F32)
            for k in keys
        ]

    ahead = scores(0)
    for i in range(blocks):
        s = ahead
        if i + 1 < blocks:
            ahead = scores(i + 1)
        at = slice(i * BLOCK, (i + 1) * BLOCK)
        tiles = [t[:, j : j + LANES] for t in s for j in range(0, t.shape[1], LANES)]
        top = tiles[0]
        for t in tiles[1:]:
            top = jnp.maximum(top, t)
        top = jnp.broadcast_to(jnp.max(top, axis=1, keepdims=True), (BLOCK, LANES))
        if not first:
            before = state[1][at, :]
            top = jnp.maximum(before, top)
        part = None
        acc = None
        n = 0
        for t, k in zip(s, keys):
            width = t.shape[1] // LANES
            probs = []
            for _ in range(width):
                p = jnp.exp2(tiles[n] - top).astype(BF16)
                probs.append(p)
                p32 = p.astype(F32)
                part = p32 if part is None else part + p32
                n += 1
            d = jnp.dot(jnp.concatenate(probs, axis=1), k[...], preferred_element_type=F32)
            acc = d if acc is None else acc + d
        if not first:
            fade = jnp.exp2(before - top)
            part = part + state[2][at, :] * fade
            acc = acc + state[0][at, :] * jnp.concatenate([fade] * (C // LANES), axis=1)
        if last:
            o = outs[0] if i * BLOCK < half else outs[1]
            to = slice((i * BLOCK) % half, (i * BLOCK) % half + BLOCK)
            o[to, 0:C] = acc
            total = jnp.broadcast_to(jnp.sum(part, axis=1, keepdims=True), (BLOCK, LANES))
            lane = lax.broadcasted_iota(jnp.int32, (BLOCK, LANES), 1)
            o[to, C : C + LANES] = jnp.where(lane < 64, top, total)
        else:
            outs[0][at, :] = acc
            outs[1][at, :] = top
            outs[2][at, :] = part


def attend(own, other, ka, kb, state, last):
    half = own.shape[0]
    first = state is None
    if last:
        outs = [jax.ShapeDtypeStruct((half, C + LANES), F32)] * 2
    else:
        outs = [
            jax.ShapeDtypeStruct((2 * half, C), F32),
            jax.ShapeDtypeStruct((2 * half, LANES), F32),
            jax.ShapeDtypeStruct((2 * half, LANES), F32),
        ]
    args = [own, other, ka, kb] + ([] if first else list(state))
    aliases = {} if first or last else {4: 0, 5: 1, 6: 2}

    def kernel(*refs):
        attend_kernel(first, last, *refs)

    flops = 4 * 2 * half * C * (ka.shape[0] + kb.shape[0])
    return call(kernel, outs, [VMEM] * len(args), args, flops, 20, aliases=aliases)


def output_kernel(a_ref, b_ref, x_ref, coef_ref, wvo_ref, hidden_ref, stats_ref):
    one = slice(C, C + 1)
    two = slice(C + LANES - 1, C + LANES)
    ma, mb = a_ref[:, one], b_ref[:, one]
    m = jnp.maximum(ma, mb)
    wa, wb = jnp.exp2(ma - m), jnp.exp2(mb - m)
    inverse = 1.0 / (a_ref[:, two] * wa + b_ref[:, two] * wb)
    mixed = a_ref[:, 0:C] * (wa * inverse) + b_ref[:, 0:C] * (wb * inverse)
    normed = (mixed * coef_ref[0:1, :] + coef_ref[1:2, :]).astype(BF16)
    hidden = x_ref[...].astype(F32) + jnp.dot(normed, wvo_ref[...], preferred_element_type=F32)
    hidden = hidden.astype(BF16)
    hidden_ref[...] = hidden
    write_stats(hidden.astype(F32), stats_ref)


def conv_kernel(
    flags_ref, h_ref, top_ref, bottom_ref, stats_ref, gain_ref, shift_ref, w_ref, bias_ref,
    out_ref, left_ref, mid_ref, right_ref,
):
    rows = h_ref.shape[0]
    scale, shift = affine(stats_ref[...], gain_ref[...], shift_ref[...], rows)

    def activate(f, at, keep):
        v = f.astype(F32) * scale + shift
        v = v / (1.0 + jnp.exp(-v))
        if keep is not None:
            v = jnp.where(keep, v, 0.0)
        column = lax.broadcasted_iota(jnp.int32, v.shape, 0) % W
        mid_ref[at : at + W, :] = v.astype(BF16)
        before = jnp.where(column == 0, 0.0, pltpu.roll(v, 1, 0))
        left_ref[at : at + W, :] = before.astype(BF16)
        after = jnp.where(column == W - 1, 0.0, pltpu.roll(v, W - 1, 0))
        right_ref[at : at + W, :] = after.astype(BF16)

    activate(top_ref[...], 0, flags_ref[0] > 0)
    for r in range(rows // W):
        activate(h_ref[r * W : (r + 1) * W, :], (r + 1) * W, None)
    activate(bottom_ref[...], rows + W, flags_ref[1] > 0)
    for r in range(0, rows, BLOCK):
        for n in range(0, C, BLOCK):
            total = None
            for dy in range(3):
                for dx, src in enumerate((left_ref, mid_ref, right_ref)):
                    d = jnp.dot(
                        src[r + dy * W : r + dy * W + BLOCK, :],
                        w_ref[3 * dy + dx, :, n : n + BLOCK],
                        preferred_element_type=F32,
                    )
                    total = d if total is None else total + d
            base = h_ref[r : r + BLOCK, n : n + BLOCK].astype(F32)
            out_ref[r : r + BLOCK, n : n + BLOCK] = (
                base + (total + bias_ref[:, n : n + BLOCK])
            ).astype(BF16)


def everyone(tile):
    count = lax.axis_size("row")
    copies = jnp.broadcast_to(tile, (count, *tile.shape))
    return lax.all_to_all(copies, "row", split_axis=0, concat_axis=0, tiled=True)


def local(
    latent, attn_gain, attn_shift, w_query, w_key, w_value, w_out,
    conv_gain, conv_shift, w_conv, conv_bias,
):
    count = lax.axis_size("row")
    chips = count // 2
    rows = latent.shape[0] * W
    half = rows // 2
    x = latent.reshape(rows, C)
    line = lambda v: v.reshape(1, C)
    swap = [(i, i ^ 1) for i in range(count)]
    turn = lambda d: [(i, ((i // 2 + d) % chips) * 2 + i % 2) for i in range(count)]

    a, b = x[:half], x[half:]
    up, down = [a, b], [a, b]
    pairs = [(a, b)]
    for step in range(1, chips // 2 + 1):
        if step < chips // 2:
            for h in range(2):
                up[h] = lax.ppermute(up[h], "row", turn(1))
                down[h] = lax.ppermute(down[h], "row", turn(-1))
                pairs.append((up[h], down[h]))
        else:
            pairs.append(
                (lax.ppermute(up[0], "row", turn(1)), lax.ppermute(down[1], "row", turn(-1)))
            )

    tile = jax.ShapeDtypeStruct((8, LANES), F32)
    wqk = lax.dot_general(
        w_query, w_key, (((1,), (1,)), ((), ())), preferred_element_type=F32
    ).astype(BF16)
    wvo = jnp.dot(w_value, w_out, preferred_element_type=F32).astype(BF16)
    stats = everyone(call(stats_kernel, tile, [VMEM], [x], 4 * rows * C))
    query, coef = call(
        query_kernel,
        [jax.ShapeDtypeStruct((rows, C), BF16), jax.ShapeDtypeStruct((8, C), F32)],
        [VMEM] * 5,
        [x, stats, line(attn_gain), line(attn_shift), wqk],
        2 * rows * C * C,
    )
    other = lax.ppermute(query, "row", swap)
    state = None
    for n, (ka, kb) in enumerate(pairs):
        state = attend(query, other, ka, kb, state, n == len(pairs) - 1)
    mine, theirs = state
    met = lax.ppermute(theirs, "row", swap)
    hidden, tile2 = call(
        output_kernel,
        [jax.ShapeDtypeStruct((rows, C), BF16), tile],
        [VMEM] * 5,
        [mine, met, x, coef, wvo],
        2 * rows * C * C,
    )
    top = lax.ppermute(hidden[rows - W :], "row", [(i, i + 1) for i in range(count - 1)])
    bottom = lax.ppermute(hidden[:W], "row", [(i + 1, i) for i in range(count - 1)])
    stats2 = everyone(tile2)
    me = lax.axis_index("row")
    flags = jnp.stack([me > 0, me < count - 1]).astype(jnp.int32)
    encoded = call(
        conv_kernel,
        jax.ShapeDtypeStruct((rows, C), BF16),
        [SMEM] + [VMEM] * 8,
        [
            flags, hidden, top, bottom, stats2, line(conv_gain), line(conv_shift),
            w_conv.reshape(9, C, C), line(conv_bias),
        ],
        18 * rows * C * C,
        scratch=[pltpu.VMEM((rows + 2 * W, C), BF16)] * 3,
    )
    return encoded.reshape(latent.shape)


def solution(mesh):
    in_specs = (P(("img", "row"), None, None), P(), P(), P(), P(), P(), P(), P(), P(), P(), P())
    out_specs = P(("img", "row"), None, None)
    return jax.shard_map(local, mesh=mesh, in_specs=in_specs, out_specs=out_specs, check_vma=False)
```

```python
import jax
import jax.numpy as jnp
from jax import lax
from jax.experimental import pallas as pl
from jax.experimental.pallas import tpu as pltpu
from jax.sharding import PartitionSpec as P


C = 512
GROUPS = 32
W = 128
LANES = 128
EPS = 1e-06
LOG2E = 1.4426950408889634
VMEM = pl.BlockSpec(memory_space=pltpu.VMEM)
SMEM = pl.BlockSpec(memory_space=pltpu.SMEM)
F32 = jnp.float32
BF16 = jnp.bfloat16
MIB = 1024 * 1024
AHEAD = 20_000_000_000


def call(kernel, outs, specs, args, flops, vmem_mib=16, scratch=(), aliases=None):
    moved = sum(a.size * a.dtype.itemsize for a in args)
    return pl.pallas_call(
        kernel,
        out_shape=outs,
        in_specs=specs,
        out_specs=jax.tree.map(lambda _: VMEM, outs),
        scratch_shapes=list(scratch),
        input_output_aliases=aliases or {},
        cost_estimate=pl.CostEstimate(flops=flops, bytes_accessed=moved, transcendentals=0),
        compiler_params=pltpu.CompilerParams(vmem_limit_bytes=vmem_mib * MIB),
    )(*args)


def group_sum(v):
    lane = lax.broadcasted_iota(jnp.int32, v.shape, 1)
    for k in (1, 2, 4, 8):
        up = pltpu.roll(v, k, 1)
        down = pltpu.roll(v, C - k, 1)
        v = v + jnp.where((lane & k) != 0, up, down)
    return v


def write_stats(field, out_ref):
    rows = field.shape[0]
    share = C // GROUPS
    mean = group_sum(jnp.broadcast_to(jnp.sum(field, 0, keepdims=True), (8, C))) * (
        1.0 / (rows * share)
    )
    offset = field - mean[0:1]
    spread = group_sum(jnp.broadcast_to(jnp.sum(offset * offset, 0, keepdims=True), (8, C)))
    for i in range(C // LANES):
        cut = slice(i * LANES, (i + 1) * LANES)
        out_ref[i : i + 1, :] = mean[0:1, cut]
        out_ref[i + 4 : i + 5, :] = spread[0:1, cut]


def affine(stats, gain, shift, rows):
    count = stats.shape[0]
    local = rows * (C // GROUPS)
    means = stats[:, 0:4, :]
    mean = jnp.sum(means, 0) * (1.0 / count)
    offset = means - mean[None]
    total = jnp.sum(stats[:, 4:8, :], 0) + local * jnp.sum(offset * offset, 0)
    inverse = lax.rsqrt(total * (1.0 / (local * count)) + EPS)
    flat = lambda v: jnp.concatenate([v[i : i + 1] for i in range(4)], axis=1)
    scale = flat(inverse) * gain
    return scale, shift - flat(mean) * scale


def stats_kernel(x_ref, out_ref):
    write_stats(x_ref[...].astype(F32), out_ref)


def fold_kernel(transposed, left_ref, right_ref, *refs):
    dims = (((1,), (1 if transposed else 0,)), ((), ()))
    product = lax.dot_general(left_ref[...], right_ref[...], dims, preferred_element_type=F32)
    refs[-1][...] = product.astype(BF16)


def fold(left, right, transposed, *early):
    def kernel(*refs):
        fold_kernel(transposed, *refs)

    args = [left, right, *early]
    out = jax.ShapeDtypeStruct((C, C), BF16)
    return call(kernel, out, [VMEM] * len(args), args, AHEAD, 8)


def query_kernel(x_ref, stats_ref, gain_ref, shift_ref, wqk_ref, q_ref, coef_ref):
    scale, shift = affine(stats_ref[...], gain_ref[...], shift_ref[...], x_ref.shape[0])
    coef_ref[0:1, :] = scale
    coef_ref[1:2, :] = shift
    normed = (x_ref[...].astype(F32) * scale + shift).astype(BF16)
    q = jnp.dot(normed, wqk_ref[...], preferred_element_type=F32)
    q_ref[...] = (q * (scale * (LOG2E / C**0.5))).astype(BF16)


BLOCK = 256


def scores_of(q, keys):
    return [
        lax.dot_general(q, k[...], (((1,), (1,)), ((), ())), preferred_element_type=F32)
        for k in keys
    ]


def wide(v):
    return jnp.concatenate([v] * (C // LANES), axis=1)


def absorb(scores, keys, state):
    tiles = [t[:, j : j + LANES] for t in scores for j in range(0, t.shape[1], LANES)]
    top = tiles[0]
    for t in tiles[1:]:
        top = jnp.maximum(top, t)
    top = jnp.broadcast_to(jnp.max(top, axis=1, keepdims=True), top.shape)
    if state is not None:
        acc0, before, part0 = state
        top = jnp.maximum(before, top)
    part = None
    acc = None
    n = 0
    for t, k in zip(scores, keys):
        probs = []
        for _ in range(t.shape[1] // LANES):
            p = jnp.exp2(tiles[n] - top).astype(BF16)
            probs.append(p)
            p32 = p.astype(F32)
            part = p32 if part is None else part + p32
            n += 1
        d = jnp.dot(jnp.concatenate(probs, axis=1), k[...], preferred_element_type=F32)
        acc = d if acc is None else acc + d
    if state is not None:
        fade = jnp.exp2(before - top)
        part = part + part0 * fade
        acc = acc + acc0 * wide(fade)
    return acc, top, part


def pack(ref, at, acc, top, part):
    ref[at, 0:C] = acc
    total = jnp.broadcast_to(jnp.sum(part, axis=1, keepdims=True), top.shape)
    lane = lax.broadcasted_iota(jnp.int32, top.shape, 1)
    ref[at, C : C + LANES] = jnp.where(lane < LANES // 2, top, total)


def attend_kernel(n_q, n_k, first, packed, *refs):
    queries, keys, refs = refs[:n_q], refs[n_q : n_q + n_k], refs[n_q + n_k :]
    if not first:
        states, refs = [refs[3 * i : 3 * i + 3] for i in range(n_q)], refs[3 * n_q :]
    work = [
        (i, slice(at, at + BLOCK)) for i in range(n_q) for at in range(0, queries[i].shape[0], BLOCK)
    ]
    ahead = scores_of(queries[0][work[0][1], :], keys)
    for n, (i, at) in enumerate(work):
        now = ahead
        if n + 1 < len(work):
            j, to = work[n + 1]
            ahead = scores_of(queries[j][to, :], keys)
        state = None if first else tuple(r[at, :] for r in states[i])
        result = absorb(now, keys, state)
        if packed and i == 1:
            pack(refs[3], at, *result)
        else:
            for ref, v in zip(refs[3 * i : 3 * i + 3], result):
                ref[at, :] = v


def attend(queries, keys, state, packed=False):
    half = queries[0].shape[0]
    first = state is None
    n_q, n_k = len(queries), len(keys)
    one = [
        jax.ShapeDtypeStruct((half, C), F32),
        jax.ShapeDtypeStruct((half, LANES), F32),
        jax.ShapeDtypeStruct((half, LANES), F32),
    ]
    outs = one * n_q
    if packed:
        outs = one + [jax.ShapeDtypeStruct((half, C + LANES), F32)]
    args = [*queries, *keys] + ([] if first else list(state))
    aliases = {} if first else {n_q + n_k + i: i for i in range(3 if packed else 3 * n_q)}

    def kernel(*refs):
        attend_kernel(n_q, n_k, first, packed, *refs)

    flops = 4 * n_q * half * C * sum(k.shape[0] for k in keys)
    return call(kernel, outs, [VMEM] * len(args), args, flops, 20, aliases=aliases)


def output_kernel(
    flags_ref, q_ref, key_ref, acc_ref, top_ref, part_ref, met_ref, x_ref, coef_ref, wvo_ref,
    hidden_ref, stats_ref, inside_ref, outside_ref,
):
    keys = [key_ref]
    rows = q_ref.shape[0]
    ahead = scores_of(q_ref[0:BLOCK, :], keys)
    for r in range(0, rows, BLOCK):
        at = slice(r, r + BLOCK)
        now = ahead
        if r + BLOCK < rows:
            ahead = scores_of(q_ref[r + BLOCK : r + 2 * BLOCK, :], keys)
        acc, top, part = absorb(now, keys, (acc_ref[at, :], top_ref[at, :], part_ref[at, :]))
        total = jnp.broadcast_to(jnp.sum(part, axis=1, keepdims=True), top.shape)
        edge = met_ref[at, C : C + LANES]
        other = jnp.broadcast_to(edge[:, 0:1], top.shape)
        other_total = jnp.broadcast_to(edge[:, LANES - 1 : LANES], top.shape)
        most = jnp.maximum(top, other)
        wa, wb = jnp.exp2(top - most), jnp.exp2(other - most)
        inverse = 1.0 / (total * wa + other_total * wb)
        mixed = acc * wide(wa * inverse) + met_ref[at, 0:C] * wide(wb * inverse)
        normed = (mixed * coef_ref[0:1, :] + coef_ref[1:2, :]).astype(BF16)
        hidden = x_ref[at, :].astype(F32) + jnp.dot(
            normed, wvo_ref[...], preferred_element_type=F32
        )
        hidden_ref[at, :] = hidden.astype(BF16)
    first = hidden_ref[0:W, :]
    last = hidden_ref[rows - W : rows, :]
    even = flags_ref[2] > 0
    inside_ref[...] = jnp.where(even, last, first)
    outside_ref[...] = jnp.where(even, first, last)
    write_stats(hidden_ref[...].astype(F32), stats_ref)


def conv_kernel(
    flags_ref, h_ref, inside_ref, outside_ref, stats_ref, gain_ref, shift_ref, w_ref, bias_ref,
    out_ref, left_ref, mid_ref, right_ref,
):
    rows = h_ref.shape[0]
    scale, shift = affine(stats_ref[...], gain_ref[...], shift_ref[...], rows)

    def activate(f, at, keep):
        v = f.astype(F32) * scale + shift
        v = v / (1.0 + jnp.exp(-v))
        if keep is not None:
            v = jnp.where(keep, v, 0.0)
        column = lax.broadcasted_iota(jnp.int32, v.shape, 0) % W
        mid_ref[at : at + W, :] = v.astype(BF16)
        before = jnp.where(column == 0, 0.0, pltpu.roll(v, 1, 0))
        left_ref[at : at + W, :] = before.astype(BF16)
        after = jnp.where(column == W - 1, 0.0, pltpu.roll(v, W - 1, 0))
        right_ref[at : at + W, :] = after.astype(BF16)

    even = flags_ref[2] > 0
    activate(jnp.where(even, outside_ref[...], inside_ref[...]), 0, flags_ref[0] > 0)
    for r in range(rows // W):
        activate(h_ref[r * W : (r + 1) * W, :], (r + 1) * W, None)
    bottom = jnp.where(even, inside_ref[...], outside_ref[...])
    activate(bottom, rows + W, flags_ref[1] > 0)
    for r in range(0, rows, BLOCK):
        for n in range(0, C, BLOCK):
            total = None
            for dy in range(3):
                for dx, src in enumerate((left_ref, mid_ref, right_ref)):
                    d = jnp.dot(
                        src[r + dy * W : r + dy * W + BLOCK, :],
                        w_ref[3 * dy + dx, :, n : n + BLOCK],
                        preferred_element_type=F32,
                    )
                    total = d if total is None else total + d
            base = h_ref[r : r + BLOCK, n : n + BLOCK].astype(F32)
            out_ref[r : r + BLOCK, n : n + BLOCK] = (
                base + (total + bias_ref[:, n : n + BLOCK])
            ).astype(BF16)


def everyone(tile):
    count = lax.axis_size("row")
    copies = jnp.broadcast_to(tile, (count, *tile.shape))
    return lax.all_to_all(copies, "row", split_axis=0, concat_axis=0, tiled=True)


def local(
    latent, attn_gain, attn_shift, w_query, w_key, w_value, w_out,
    conv_gain, conv_shift, w_conv, conv_bias,
):
    count = lax.axis_size("row")
    chips = count // 2
    rows = latent.shape[0] * W
    me = lax.axis_index("row")
    flags = jnp.stack([me > 0, me < count - 1, me % 2 == 0]).astype(jnp.int32)
    latent, flags = lax.optimization_barrier((latent, flags))
    x = latent.reshape(rows, C)
    line = lambda v: v.reshape(1, C)
    swap = [(i, i ^ 1) for i in range(count)]
    ring = [(i, ((i // 2 + 1 - 2 * (i % 2)) % chips) * 2 + i % 2) for i in range(count)]

    move = lambda v, to: lax.ppermute(v, "row", to)
    tile = jax.ShapeDtypeStruct((8, LANES), F32)
    stats = call(stats_kernel, tile, [VMEM], [x], AHEAD)
    wqk = fold(w_query, w_key, True)
    taps = w_conv.reshape(9, C, C)
    wvo = fold(w_value, w_out, False, taps)
    near, far = x, move(x, swap)
    pieces = [x]
    for step in range(1, chips // 2 + 1):
        near = move(near, ring)
        pieces.append(near)
        if step < chips // 2:
            far = move(far, ring)
            pieces.append(far)

    stats = everyone(stats)
    query, coef = call(
        query_kernel,
        [jax.ShapeDtypeStruct((rows, C), BF16), jax.ShapeDtypeStruct((8, C), F32)],
        [VMEM] * 5,
        [x, stats, line(attn_gain), line(attn_shift), wqk],
        2 * rows * C * C,
    )
    other = move(query, swap)
    state = None
    *early, late = pieces
    for n, key in enumerate(early):
        state = attend([query, other], [key], state, n == len(early) - 1)
    *mine, theirs = state
    met = move(theirs, swap)
    across = move(late, swap)
    mine = attend([query], [late], mine)
    edge = jax.ShapeDtypeStruct((W, C), BF16)
    hidden, tile2, inside, outside = call(
        output_kernel,
        [jax.ShapeDtypeStruct((rows, C), BF16), tile, edge, edge],
        [SMEM] + [VMEM] * 9,
        [flags, query, across, *mine, met, x, coef, wvo],
        6 * rows * C * C,
        20,
    )
    between = [(i, i + 1) for i in range(1, count - 1, 2)]
    inside = move(inside, swap)
    outside = move(outside, between + [(b, a) for a, b in between])
    stats2 = everyone(tile2)
    encoded = call(
        conv_kernel,
        jax.ShapeDtypeStruct((rows, C), BF16),
        [SMEM] + [VMEM] * 8,
        [
            flags, hidden, inside, outside, stats2, line(conv_gain), line(conv_shift),
            taps, line(conv_bias),
        ],
        18 * rows * C * C,
        scratch=[pltpu.VMEM((rows + 2 * W, C), BF16)] * 3,
    )
    return encoded.reshape(latent.shape)


def solution(mesh):
    in_specs = (P(("img", "row"), None, None), P(), P(), P(), P(), P(), P(), P(), P(), P(), P())
    out_specs = P(("img", "row"), None, None)
    return jax.shard_map(local, mesh=mesh, in_specs=in_specs, out_specs=out_specs, check_vma=False)
```

```python
import jax
import jax.numpy as jnp
from jax import lax
from jax.experimental import pallas as pl
from jax.experimental.pallas import tpu as pltpu
from jax.sharding import PartitionSpec as P


C = 512
GROUPS = 32
W = 128
LANES = 128
EPS = 1e-06
LOG2E = 1.4426950408889634
VMEM = pl.BlockSpec(memory_space=pltpu.VMEM)
SMEM = pl.BlockSpec(memory_space=pltpu.SMEM)
F32 = jnp.float32
BF16 = jnp.bfloat16
MIB = 1024 * 1024
AHEAD = 20_000_000_000


def call(kernel, outs, specs, args, flops, vmem_mib=16, scratch=(), aliases=None):
    moved = sum(a.size * a.dtype.itemsize for a in args)
    return pl.pallas_call(
        kernel,
        out_shape=outs,
        in_specs=specs,
        out_specs=jax.tree.map(lambda _: VMEM, outs),
        scratch_shapes=list(scratch),
        input_output_aliases=aliases or {},
        cost_estimate=pl.CostEstimate(flops=flops, bytes_accessed=moved, transcendentals=0),
        compiler_params=pltpu.CompilerParams(vmem_limit_bytes=vmem_mib * MIB),
    )(*args)


def group_sum(v):
    lane = lax.broadcasted_iota(jnp.int32, v.shape, 1)
    for k in (1, 2, 4, 8):
        up = pltpu.roll(v, k, 1)
        down = pltpu.roll(v, C - k, 1)
        v = v + jnp.where((lane & k) != 0, up, down)
    return v


def write_stats(field, out_ref):
    rows = field.shape[0]
    share = C // GROUPS
    mean = group_sum(jnp.broadcast_to(jnp.sum(field, 0, keepdims=True), (8, C))) * (
        1.0 / (rows * share)
    )
    offset = field - mean[0:1]
    spread = group_sum(jnp.broadcast_to(jnp.sum(offset * offset, 0, keepdims=True), (8, C)))
    for i in range(C // LANES):
        cut = slice(i * LANES, (i + 1) * LANES)
        out_ref[i : i + 1, :] = mean[0:1, cut]
        out_ref[i + 4 : i + 5, :] = spread[0:1, cut]


def affine(stats, gain, shift, rows):
    count = stats.shape[0]
    local = rows * (C // GROUPS)
    means = stats[:, 0:4, :]
    mean = jnp.sum(means, 0) * (1.0 / count)
    offset = means - mean[None]
    total = jnp.sum(stats[:, 4:8, :], 0) + local * jnp.sum(offset * offset, 0)
    inverse = lax.rsqrt(total * (1.0 / (local * count)) + EPS)
    flat = lambda v: jnp.concatenate([v[i : i + 1] for i in range(4)], axis=1)
    scale = flat(inverse) * gain
    return scale, shift - flat(mean) * scale


def stats_kernel(x_ref, out_ref):
    write_stats(x_ref[...].astype(F32), out_ref)


def fold_kernel(transposed, left_ref, right_ref, *refs):
    dims = (((1,), (1 if transposed else 0,)), ((), ()))
    product = lax.dot_general(left_ref[...], right_ref[...], dims, preferred_element_type=F32)
    refs[-1][...] = product.astype(BF16)


def fold(left, right, transposed, *early):
    def kernel(*refs):
        fold_kernel(transposed, *refs)

    args = [left, right, *early]
    out = jax.ShapeDtypeStruct((C, C), BF16)
    return call(kernel, out, [VMEM] * len(args), args, AHEAD, 8)


def query_kernel(
    flags_ref, x_ref, far_ref, stats_ref, gain_ref, shift_ref, wqk_ref, q_ref, coef_ref, halo_ref
):
    rows = x_ref.shape[0]
    scale, shift = affine(stats_ref[...], gain_ref[...], shift_ref[...], rows)
    coef_ref[0:1, :] = scale
    coef_ref[1:2, :] = shift
    halo = jnp.where(flags_ref[2] > 0, far_ref[rows - W : rows, :], far_ref[0:W, :])
    halo_ref[...] = halo
    for x, at in ((x_ref[...], slice(0, rows)), (halo, slice(rows, rows + W))):
        normed = (x.astype(F32) * scale + shift).astype(BF16)
        q = jnp.dot(normed, wqk_ref[...], preferred_element_type=F32)
        q_ref[at, :] = (q * (scale * (LOG2E / C**0.5))).astype(BF16)


BLOCK = 320
TILE = 256


def scores_of(q, keys):
    return [
        lax.dot_general(q, k[...], (((1,), (1,)), ((), ())), preferred_element_type=F32)
        for k in keys
    ]


def wide(v):
    return jnp.concatenate([v] * (C // LANES), axis=1)


def absorb(scores, keys, state):
    tiles = [t[:, j : j + LANES] for t in scores for j in range(0, t.shape[1], LANES)]
    top = tiles[0]
    for t in tiles[1:]:
        top = jnp.maximum(top, t)
    top = jnp.broadcast_to(jnp.max(top, axis=1, keepdims=True), top.shape)
    if state is not None:
        acc0, before, part0 = state
        top = jnp.maximum(before, top)
    part = None
    acc = None
    n = 0
    for t, k in zip(scores, keys):
        probs = []
        for _ in range(t.shape[1] // LANES):
            p = jnp.exp2(tiles[n] - top).astype(BF16)
            probs.append(p)
            p32 = p.astype(F32)
            part = p32 if part is None else part + p32
            n += 1
        d = jnp.dot(jnp.concatenate(probs, axis=1), k[...], preferred_element_type=F32)
        acc = d if acc is None else acc + d
    if state is not None:
        fade = jnp.exp2(before - top)
        part = part + part0 * fade
        acc = acc + acc0 * wide(fade)
    return acc, top, part


def pack(ref, at, acc, top, part):
    ref[at, 0:C] = acc
    total = jnp.broadcast_to(jnp.sum(part, axis=1, keepdims=True), top.shape)
    lane = lax.broadcasted_iota(jnp.int32, top.shape, 1)
    ref[at, C : C + LANES] = jnp.where(lane < LANES // 2, top, total)


def attend_kernel(n_q, n_k, first, packed, *refs):
    queries, keys, refs = refs[:n_q], refs[n_q : n_q + n_k], refs[n_q + n_k :]
    if not first:
        states, refs = [refs[3 * i : 3 * i + 3] for i in range(n_q)], refs[3 * n_q :]
    work = [
        (i, slice(at, at + BLOCK)) for i in range(n_q) for at in range(0, queries[i].shape[0], BLOCK)
    ]
    ahead = scores_of(queries[0][work[0][1], :], keys)
    for n, (i, at) in enumerate(work):
        now = ahead
        if n + 1 < len(work):
            j, to = work[n + 1]
            ahead = scores_of(queries[j][to, :], keys)
        state = None if first else tuple(r[at, :] for r in states[i])
        result = absorb(now, keys, state)
        if packed and i == 1:
            pack(refs[3], at, *result)
        else:
            for ref, v in zip(refs[3 * i : 3 * i + 3], result):
                ref[at, :] = v


def attend(queries, keys, state, packed=False):
    half = queries[0].shape[0]
    first = state is None
    n_q, n_k = len(queries), len(keys)
    one = [
        jax.ShapeDtypeStruct((half, C), F32),
        jax.ShapeDtypeStruct((half, LANES), F32),
        jax.ShapeDtypeStruct((half, LANES), F32),
    ]
    outs = one * n_q
    if packed:
        outs = one + [jax.ShapeDtypeStruct((half, C + LANES), F32)]
    args = [*queries, *keys] + ([] if first else list(state))
    aliases = {} if first else {n_q + n_k + i: i for i in range(3 if packed else 3 * n_q)}

    def kernel(*refs):
        attend_kernel(n_q, n_k, first, packed, *refs)

    flops = 4 * n_q * half * C * sum(k.shape[0] for k in keys)
    return call(kernel, outs, [VMEM] * len(args), args, flops, 20, aliases=aliases)


def output_kernel(
    flags_ref, q_ref, key_ref, acc_ref, top_ref, part_ref, met_ref, x_ref, halo_ref, coef_ref,
    wvo_ref, hidden_ref, stats_ref, inside_ref, outside_ref,
):
    keys = [key_ref]
    rows = x_ref.shape[0]
    half = rows // 2
    blocks = [slice(0, half), slice(half, rows), slice(rows, rows + W)]
    ahead = scores_of(q_ref[blocks[0], :], keys)
    for n, at in enumerate(blocks):
        now = ahead
        if n + 1 < len(blocks):
            ahead = scores_of(q_ref[blocks[n + 1], :], keys)
        acc, top, part = absorb(now, keys, (acc_ref[at, :], top_ref[at, :], part_ref[at, :]))
        total = jnp.broadcast_to(jnp.sum(part, axis=1, keepdims=True), top.shape)
        edge = met_ref[at, C : C + LANES]
        other = jnp.broadcast_to(edge[:, 0:1], top.shape)
        other_total = jnp.broadcast_to(edge[:, LANES - 1 : LANES], top.shape)
        most = jnp.maximum(top, other)
        wa, wb = jnp.exp2(top - most), jnp.exp2(other - most)
        inverse = 1.0 / (total * wa + other_total * wb)
        mixed = acc * wide(wa * inverse) + met_ref[at, 0:C] * wide(wb * inverse)
        normed = (mixed * coef_ref[0:1, :] + coef_ref[1:2, :]).astype(BF16)
        x = halo_ref[...] if at.start == rows else x_ref[at, :]
        hidden = x.astype(F32) + jnp.dot(normed, wvo_ref[...], preferred_element_type=F32)
        if at.start == rows:
            outside_ref[...] = hidden.astype(BF16)
        else:
            hidden_ref[at, :] = hidden.astype(BF16)
    inside_ref[...] = jnp.where(
        flags_ref[2] > 0, hidden_ref[rows - W : rows, :], hidden_ref[0:W, :]
    )
    write_stats(hidden_ref[...].astype(F32), stats_ref)


def conv_kernel(
    flags_ref, h_ref, inside_ref, outside_ref, stats_ref, gain_ref, shift_ref, w_ref, bias_ref,
    out_ref, left_ref, mid_ref, right_ref,
):
    rows = h_ref.shape[0]
    scale, shift = affine(stats_ref[...], gain_ref[...], shift_ref[...], rows)

    def activate(f, at, keep):
        v = f.astype(F32) * scale + shift
        v = v / (1.0 + jnp.exp(-v))
        if keep is not None:
            v = jnp.where(keep, v, 0.0)
        column = lax.broadcasted_iota(jnp.int32, v.shape, 0) % W
        mid_ref[at : at + W, :] = v.astype(BF16)
        before = jnp.where(column == 0, 0.0, pltpu.roll(v, 1, 0))
        left_ref[at : at + W, :] = before.astype(BF16)
        after = jnp.where(column == W - 1, 0.0, pltpu.roll(v, W - 1, 0))
        right_ref[at : at + W, :] = after.astype(BF16)

    even = flags_ref[2] > 0
    activate(jnp.where(even, outside_ref[...], inside_ref[...]), 0, flags_ref[0] > 0)
    for r in range(rows // W):
        activate(h_ref[r * W : (r + 1) * W, :], (r + 1) * W, None)
    bottom = jnp.where(even, inside_ref[...], outside_ref[...])
    activate(bottom, rows + W, flags_ref[1] > 0)
    for r in range(0, rows, TILE):
        for n in range(0, C, TILE):
            total = None
            for dy in range(3):
                for dx, src in enumerate((left_ref, mid_ref, right_ref)):
                    d = jnp.dot(
                        src[r + dy * W : r + dy * W + TILE, :],
                        w_ref[3 * dy + dx, :, n : n + TILE],
                        preferred_element_type=F32,
                    )
                    total = d if total is None else total + d
            base = h_ref[r : r + TILE, n : n + TILE].astype(F32)
            out_ref[r : r + TILE, n : n + TILE] = (
                base + (total + bias_ref[:, n : n + TILE])
            ).astype(BF16)


def everyone(tile):
    count = lax.axis_size("row")
    copies = jnp.broadcast_to(tile, (count, *tile.shape))
    return lax.all_to_all(copies, "row", split_axis=0, concat_axis=0, tiled=True)


def local(
    latent, attn_gain, attn_shift, w_query, w_key, w_value, w_out,
    conv_gain, conv_shift, w_conv, conv_bias,
):
    count = lax.axis_size("row")
    chips = count // 2
    rows = latent.shape[0] * W
    me = lax.axis_index("row")
    flags = jnp.stack([me > 0, me < count - 1, me % 2 == 0]).astype(jnp.int32)
    latent, flags = lax.optimization_barrier((latent, flags))
    x = latent.reshape(rows, C)
    line = lambda v: v.reshape(1, C)
    swap = [(i, i ^ 1) for i in range(count)]
    ring = [(i, ((i // 2 + 1 - 2 * (i % 2)) % chips) * 2 + i % 2) for i in range(count)]

    move = lambda v, to: lax.ppermute(v, "row", to)
    tile = jax.ShapeDtypeStruct((8, LANES), F32)
    stats = call(stats_kernel, tile, [VMEM], [x], AHEAD)
    wqk = fold(w_query, w_key, True)
    taps = w_conv.reshape(9, C, C)
    wvo = fold(w_value, w_out, False, taps)
    near, far = x, move(x, swap)
    pieces = [x]
    for step in range(1, chips // 2 + 1):
        near = move(near, ring)
        pieces.append(near)
        if step < chips // 2:
            far = move(far, ring)
            pieces.append(far)

    stats = everyone(stats)
    query, coef, halo = call(
        query_kernel,
        [
            jax.ShapeDtypeStruct((rows + W, C), BF16),
            jax.ShapeDtypeStruct((8, C), F32),
            jax.ShapeDtypeStruct((W, C), BF16),
        ],
        [SMEM] + [VMEM] * 6,
        [flags, x, pieces[2], stats, line(attn_gain), line(attn_shift), wqk],
        2 * rows * C * C,
    )
    other = move(query, swap)
    state = None
    *early, late = pieces
    for n, key in enumerate(early):
        state = attend([query, other], [key], state, n == len(early) - 1)
    *mine, theirs = state
    met = move(theirs, swap)
    across = move(late, swap)
    mine = attend([query], [late], mine)
    edge = jax.ShapeDtypeStruct((W, C), BF16)
    hidden, tile2, inside, outside = call(
        output_kernel,
        [jax.ShapeDtypeStruct((rows, C), BF16), tile, edge, edge],
        [SMEM] + [VMEM] * 10,
        [flags, query, across, *mine, met, x, halo, coef, wvo],
        6 * rows * C * C,
        20,
    )
    inside = move(inside, swap)
    stats2 = everyone(tile2)
    encoded = call(
        conv_kernel,
        jax.ShapeDtypeStruct((rows, C), BF16),
        [SMEM] + [VMEM] * 8,
        [
            flags, hidden, inside, outside, stats2, line(conv_gain), line(conv_shift),
            taps, line(conv_bias),
        ],
        18 * rows * C * C,
        scratch=[pltpu.VMEM((rows + 2 * W, C), BF16)] * 3,
    )
    return encoded.reshape(latent.shape)


def solution(mesh):
    in_specs = (P(("img", "row"), None, None), P(), P(), P(), P(), P(), P(), P(), P(), P(), P())
    out_specs = P(("img", "row"), None, None)
    return jax.shard_map(local, mesh=mesh, in_specs=in_specs, out_specs=out_specs, check_vma=False)
```

```python
import jax
import jax.numpy as jnp
from jax import lax
from jax.experimental import pallas as pl
from jax.experimental.pallas import tpu as pltpu
from jax.sharding import PartitionSpec as P


C = 512
GROUPS = 32
W = 128
LANES = 128
EPS = 1e-06
LOG2E = 1.4426950408889634
VMEM = pl.BlockSpec(memory_space=pltpu.VMEM)
F32 = jnp.float32
BF16 = jnp.bfloat16
MIB = 1024 * 1024
AHEAD = 20_000_000_000


def call(kernel, outs, specs, args, flops, vmem_mib=16, scratch=(), aliases=None):
    moved = sum(a.size * a.dtype.itemsize for a in args)
    return pl.pallas_call(
        kernel,
        out_shape=outs,
        in_specs=specs,
        out_specs=jax.tree.map(lambda _: VMEM, outs),
        scratch_shapes=list(scratch),
        input_output_aliases=aliases or {},
        cost_estimate=pl.CostEstimate(flops=flops, bytes_accessed=moved, transcendentals=0),
        compiler_params=pltpu.CompilerParams(vmem_limit_bytes=vmem_mib * MIB),
    )(*args)


def group_sum(v):
    lane = lax.broadcasted_iota(jnp.int32, v.shape, 1)
    for k in (1, 2, 4, 8):
        up = pltpu.roll(v, k, 1)
        down = pltpu.roll(v, C - k, 1)
        v = v + jnp.where((lane & k) != 0, up, down)
    return v


def store_stats(mean, spread, out_ref):
    for i in range(C // LANES):
        cut = slice(i * LANES, (i + 1) * LANES)
        out_ref[i : i + 1, :] = mean[0:1, cut]
        out_ref[i + 4 : i + 5, :] = spread[0:1, cut]


def field_stats(parts, out_ref):
    share = C // GROUPS
    first = jnp.sum(parts[0], 0, keepdims=True) * (1.0 / (parts[0].shape[0] * share))
    pivot = group_sum(jnp.broadcast_to(first, (8, C)))[0:1]
    one = two = None
    for part in parts:
        offset = part - pivot
        sums = jnp.sum(offset, 0, keepdims=True), jnp.sum(offset * offset, 0, keepdims=True)
        one, two = sums if one is None else (one + sums[0], two + sums[1])
    row = lax.broadcasted_iota(jnp.int32, (8, C), 0)
    total = group_sum(jnp.where(row == 0, one, two))
    drift = total[0:1] * (1.0 / (sum(p.shape[0] for p in parts) * share))
    spread = jnp.maximum(total[1:2] - total[0:1] * drift, 0.0)
    store_stats(pivot + drift, spread, out_ref)


def affine(stats, gain, shift, rows):
    count = stats.shape[0]
    local = rows * (C // GROUPS)
    means = stats[:, 0:4, :]
    mean = jnp.sum(means, 0) * (1.0 / count)
    offset = means - mean[None]
    total = jnp.sum(stats[:, 4:8, :], 0) + local * jnp.sum(offset * offset, 0)
    inverse = lax.rsqrt(total * (1.0 / (local * count)) + EPS)
    flat = lambda v: jnp.concatenate([v[i : i + 1] for i in range(4)], axis=1)
    scale = flat(inverse) * gain
    return scale, shift - flat(mean) * scale


def pick(flags_ref, row, yes, no):
    flag = flags_ref[row : row + 1, :]
    wanted = jnp.broadcast_to(jnp.concatenate([flag] * (C // LANES), axis=1), yes.shape) > 0.0
    return jnp.where(wanted, yes, no)


def stats_kernel(x_ref, out_ref):
    half = x_ref.shape[0] // 2
    field_stats([x_ref[:half, :].astype(F32), x_ref[half:, :].astype(F32)], out_ref)


def fold_kernel(transposed, left_ref, right_ref, *refs):
    dims = (((1,), (1 if transposed else 0,)), ((), ()))
    product = lax.dot_general(left_ref[...], right_ref[...], dims, preferred_element_type=F32)
    refs[-1][...] = product.astype(BF16)


def fold(left, right, transposed, *early):
    def kernel(*refs):
        fold_kernel(transposed, *refs)

    args = [left, right, *early]
    out = jax.ShapeDtypeStruct((C, C), BF16)
    return call(kernel, out, [VMEM] * len(args), args, AHEAD, 8)


def query_kernel(
    flags_ref, x_ref, far_ref, stats_ref, gain_ref, shift_ref, wqk_ref, q_ref, coef_ref, halo_ref
):
    rows = x_ref.shape[0]
    scale, shift = affine(stats_ref[...], gain_ref[...], shift_ref[...], rows)
    coef_ref[0:1, :] = scale
    coef_ref[1:2, :] = shift
    halo = pick(flags_ref, 2, far_ref[rows - W : rows, :], far_ref[0:W, :])
    halo_ref[...] = halo
    for x, at in ((x_ref[...], slice(0, rows)), (halo, slice(rows, rows + W))):
        normed = (x.astype(F32) * scale + shift).astype(BF16)
        q = jnp.dot(normed, wqk_ref[...], preferred_element_type=F32)
        q_ref[at, :] = (q * (scale * (LOG2E / C**0.5))).astype(BF16)


BLOCK = 320
TILE = 256


def scores_of(q, keys):
    return [
        lax.dot_general(q, k[...], (((1,), (1,)), ((), ())), preferred_element_type=F32)
        for k in keys
    ]


def wide(v):
    return jnp.concatenate([v] * (C // LANES), axis=1)


def absorb(scores, keys, state):
    tiles = [t[:, j : j + LANES] for t in scores for j in range(0, t.shape[1], LANES)]
    top = tiles[0]
    for t in tiles[1:]:
        top = jnp.maximum(top, t)
    top = jnp.broadcast_to(jnp.max(top, axis=1, keepdims=True), top.shape)
    if state is not None:
        acc0, before, part0 = state
        top = jnp.maximum(before, top)
    part = None
    acc = None
    n = 0
    for t, k in zip(scores, keys):
        probs = []
        for _ in range(t.shape[1] // LANES):
            p = jnp.exp2(tiles[n] - top).astype(BF16)
            probs.append(p)
            p32 = p.astype(F32)
            part = p32 if part is None else part + p32
            n += 1
        d = jnp.dot(jnp.concatenate(probs, axis=1), k[...], preferred_element_type=F32)
        acc = d if acc is None else acc + d
    if state is not None:
        fade = jnp.exp2(before - top)
        part = part + part0 * fade
        acc = acc + acc0 * wide(fade)
    return acc, top, part


def pack(ref, at, acc, top, part):
    ref[at, 0:C] = acc
    total = jnp.broadcast_to(jnp.sum(part, axis=1, keepdims=True), top.shape)
    lane = lax.broadcasted_iota(jnp.int32, top.shape, 1)
    ref[at, C : C + LANES] = jnp.where(lane < LANES // 2, top, total)


def attend_kernel(n_q, n_k, first, packed, *refs):
    queries, keys, refs = refs[:n_q], refs[n_q : n_q + n_k], refs[n_q + n_k :]
    if not first:
        states, refs = [refs[3 * i : 3 * i + 3] for i in range(n_q)], refs[3 * n_q :]
    work = [
        (i, slice(at, at + BLOCK)) for i in range(n_q) for at in range(0, queries[i].shape[0], BLOCK)
    ]
    ahead = scores_of(queries[0][work[0][1], :], keys)
    for n, (i, at) in enumerate(work):
        now = ahead
        if n + 1 < len(work):
            j, to = work[n + 1]
            ahead = scores_of(queries[j][to, :], keys)
        state = None if first else tuple(r[at, :] for r in states[i])
        result = absorb(now, keys, state)
        if packed and i == 1:
            pack(refs[3], at, *result)
        else:
            for ref, v in zip(refs[3 * i : 3 * i + 3], result):
                ref[at, :] = v


def attend(queries, keys, state, packed=False):
    half = queries[0].shape[0]
    first = state is None
    n_q, n_k = len(queries), len(keys)
    one = [
        jax.ShapeDtypeStruct((half, C), F32),
        jax.ShapeDtypeStruct((half, LANES), F32),
        jax.ShapeDtypeStruct((half, LANES), F32),
    ]
    outs = one * n_q
    if packed:
        outs = one + [jax.ShapeDtypeStruct((half, C + LANES), F32)]
    args = [*queries, *keys] + ([] if first else list(state))
    aliases = {} if first else {n_q + n_k + i: i for i in range(3 if packed else 3 * n_q)}

    def kernel(*refs):
        attend_kernel(n_q, n_k, first, packed, *refs)

    flops = 4 * n_q * half * C * sum(k.shape[0] for k in keys)
    return call(kernel, outs, [VMEM] * len(args), args, flops, 20, aliases=aliases)


def output_kernel(
    flags_ref, q_ref, key_ref, acc_ref, top_ref, part_ref, met_ref, x_ref, halo_ref, coef_ref,
    wvo_ref, hidden_ref, stats_ref, inside_ref, outside_ref,
):
    keys = [key_ref]
    rows = x_ref.shape[0]
    half = rows // 2
    blocks = [slice(0, half), slice(half, rows), slice(rows, rows + W)]
    parts = []
    ahead = scores_of(q_ref[blocks[0], :], keys)
    for n, at in enumerate(blocks):
        now = ahead
        if n + 1 < len(blocks):
            ahead = scores_of(q_ref[blocks[n + 1], :], keys)
        acc, top, part = absorb(now, keys, (acc_ref[at, :], top_ref[at, :], part_ref[at, :]))
        total = jnp.broadcast_to(jnp.sum(part, axis=1, keepdims=True), top.shape)
        edge = met_ref[at, C : C + LANES]
        other = jnp.broadcast_to(edge[:, 0:1], top.shape)
        other_total = jnp.broadcast_to(edge[:, LANES - 1 : LANES], top.shape)
        most = jnp.maximum(top, other)
        wa, wb = jnp.exp2(top - most), jnp.exp2(other - most)
        inverse = 1.0 / (total * wa + other_total * wb)
        mixed = acc * wide(wa * inverse) + met_ref[at, 0:C] * wide(wb * inverse)
        normed = (mixed * coef_ref[0:1, :] + coef_ref[1:2, :]).astype(BF16)
        x = halo_ref[...] if at.start == rows else x_ref[at, :]
        hidden = x.astype(F32) + jnp.dot(normed, wvo_ref[...], preferred_element_type=F32)
        if at.start == rows:
            outside_ref[...] = hidden.astype(BF16)
        else:
            hidden_ref[at, :] = hidden.astype(BF16)
            parts.append(hidden.astype(BF16).astype(F32))
        if n == 1:
            field_stats(parts, stats_ref)
    inside_ref[...] = pick(
        flags_ref, 2, hidden_ref[rows - W : rows, :], hidden_ref[0:W, :]
    )


def conv_kernel(
    flags_ref, h_ref, inside_ref, outside_ref, stats_ref, gain_ref, shift_ref, w_ref, bias_ref,
    out_ref, left_ref, mid_ref, right_ref,
):
    rows = h_ref.shape[0]
    scale, shift = affine(stats_ref[...], gain_ref[...], shift_ref[...], rows)
    scale, shift = 0.5 * scale, 0.5 * shift

    def activate(f, at, keep):
        v = f.astype(F32) * scale + shift
        v = v + v * jnp.tanh(v)
        if keep is not None:
            v = pick(flags_ref, keep, v, jnp.zeros_like(v))
        column = lax.broadcasted_iota(jnp.int32, v.shape, 0) % W
        mid_ref[at : at + W, :] = v.astype(BF16)
        before = jnp.where(column == 0, 0.0, pltpu.roll(v, 1, 0))
        left_ref[at : at + W, :] = before.astype(BF16)
        after = jnp.where(column == W - 1, 0.0, pltpu.roll(v, W - 1, 0))
        right_ref[at : at + W, :] = after.astype(BF16)

    inside, outside = inside_ref[...].astype(F32), outside_ref[...].astype(F32)
    activate(pick(flags_ref, 2, outside, inside), 0, 0)
    for r in range(rows // W):
        activate(h_ref[r * W : (r + 1) * W, :], (r + 1) * W, None)
    activate(pick(flags_ref, 2, inside, outside), rows + W, 1)
    for r in range(0, rows, TILE):
        for n in range(0, C, TILE):
            total = None
            for dy in range(3):
                for dx, src in enumerate((left_ref, mid_ref, right_ref)):
                    d = jnp.dot(
                        src[r + dy * W : r + dy * W + TILE, :],
                        w_ref[3 * dy + dx, :, n : n + TILE],
                        preferred_element_type=F32,
                    )
                    total = d if total is None else total + d
            base = h_ref[r : r + TILE, n : n + TILE].astype(F32)
            out_ref[r : r + TILE, n : n + TILE] = (
                base + (total + bias_ref[:, n : n + TILE])
            ).astype(BF16)


def everyone(tile):
    count = lax.axis_size("row")
    copies = jnp.broadcast_to(tile, (count, *tile.shape))
    return lax.all_to_all(copies, "row", split_axis=0, concat_axis=0, tiled=True)


def local(
    latent, attn_gain, attn_shift, w_query, w_key, w_value, w_out,
    conv_gain, conv_shift, w_conv, conv_bias,
):
    count = lax.axis_size("row")
    chips = count // 2
    rows = latent.shape[0] * W
    me = lax.axis_index("row")
    place = lax.broadcasted_iota(jnp.int32, (8, LANES), 0)
    holds = [me > 0, me < count - 1, me % 2 == 0]
    flags = sum(jnp.where((place == i) & h, 1.0, 0.0) for i, h in enumerate(holds))
    latent, flags = lax.optimization_barrier((latent, flags))
    x = latent.reshape(rows, C)
    line = lambda v: v.reshape(1, C)
    swap = [(i, i ^ 1) for i in range(count)]
    ring = [(i, ((i // 2 + 1 - 2 * (i % 2)) % chips) * 2 + i % 2) for i in range(count)]

    move = lambda v, to: lax.ppermute(v, "row", to)
    tile = jax.ShapeDtypeStruct((8, LANES), F32)
    stats = call(stats_kernel, tile, [VMEM], [x], AHEAD)
    wqk = fold(w_query, w_key, True)
    taps = w_conv.reshape(9, C, C)
    wvo = fold(w_value, w_out, False, taps)
    near, far = x, move(x, swap)
    pieces = [x]
    for step in range(1, chips // 2 + 1):
        near = move(near, ring)
        pieces.append(near)
        if step < chips // 2:
            far = move(far, ring)
            pieces.append(far)

    stats = everyone(stats)
    query, coef, halo = call(
        query_kernel,
        [
            jax.ShapeDtypeStruct((rows + W, C), BF16),
            jax.ShapeDtypeStruct((8, C), F32),
            jax.ShapeDtypeStruct((W, C), BF16),
        ],
        [VMEM] * 7,
        [flags, x, pieces[2], stats, line(attn_gain), line(attn_shift), wqk],
        2 * rows * C * C,
    )
    other = move(query, swap)
    state = None
    *early, late = pieces
    for n, key in enumerate(early):
        state = attend([query, other], [key], state, n == len(early) - 1)
    *mine, theirs = state
    met = move(theirs, swap)
    across = move(late, swap)
    mine = attend([query], [late], mine)
    edge = jax.ShapeDtypeStruct((W, C), BF16)
    hidden, tile2, inside, outside = call(
        output_kernel,
        [jax.ShapeDtypeStruct((rows, C), BF16), tile, edge, edge],
        [VMEM] * 11,
        [flags, query, across, *mine, met, x, halo, coef, wvo],
        6 * rows * C * C,
        20,
    )
    inside = move(inside, swap)
    stats2 = everyone(tile2)
    encoded = call(
        conv_kernel,
        jax.ShapeDtypeStruct((rows, C), BF16),
        [VMEM] * 9,
        [
            flags, hidden, inside, outside, stats2, line(conv_gain), line(conv_shift),
            taps, line(conv_bias),
        ],
        18 * rows * C * C,
        scratch=[pltpu.VMEM((rows + 2 * W, C), BF16)] * 3,
    )
    return encoded.reshape(latent.shape)


def solution(mesh):
    in_specs = (P(("img", "row"), None, None), P(), P(), P(), P(), P(), P(), P(), P(), P(), P())
    out_specs = P(("img", "row"), None, None)
    return jax.shard_map(local, mesh=mesh, in_specs=in_specs, out_specs=out_specs, check_vma=False)
```

```python
import jax
import jax.numpy as jnp
from jax import lax
from jax.experimental import pallas as pl
from jax.experimental.pallas import tpu as pltpu
from jax.sharding import PartitionSpec as P


C = 512
GROUPS = 32
W = 128
LANES = 128
EPS = 1e-06
LOG2E = 1.4426950408889634
VMEM = pl.BlockSpec(memory_space=pltpu.VMEM)
F32 = jnp.float32
BF16 = jnp.bfloat16
MIB = 1024 * 1024
AHEAD = 20_000_000_000


def call(kernel, outs, specs, args, flops, vmem_mib=16, scratch=(), aliases=None):
    moved = sum(a.size * a.dtype.itemsize for a in args)
    return pl.pallas_call(
        kernel,
        out_shape=outs,
        in_specs=specs,
        out_specs=jax.tree.map(lambda _: VMEM, outs),
        scratch_shapes=list(scratch),
        input_output_aliases=aliases or {},
        cost_estimate=pl.CostEstimate(flops=flops, bytes_accessed=moved, transcendentals=0),
        compiler_params=pltpu.CompilerParams(vmem_limit_bytes=vmem_mib * MIB),
    )(*args)


def group_sum(v):
    lane = lax.broadcasted_iota(jnp.int32, v.shape, 1)
    for k in (1, 2, 4, 8):
        up = pltpu.roll(v, k, 1)
        down = pltpu.roll(v, C - k, 1)
        v = v + jnp.where((lane & k) != 0, up, down)
    return v


def store_stats(mean, spread, out_ref):
    for i in range(C // LANES):
        cut = slice(i * LANES, (i + 1) * LANES)
        out_ref[i : i + 1, :] = mean[0:1, cut]
        out_ref[i + 4 : i + 5, :] = spread[0:1, cut]


def field_stats(parts, out_ref):
    share = C // GROUPS
    first = jnp.sum(parts[0], 0, keepdims=True) * (1.0 / (parts[0].shape[0] * share))
    pivot = group_sum(jnp.broadcast_to(first, (8, C)))[0:1]
    one = two = None
    for part in parts:
        offset = part - pivot
        sums = jnp.sum(offset, 0, keepdims=True), jnp.sum(offset * offset, 0, keepdims=True)
        one, two = sums if one is None else (one + sums[0], two + sums[1])
    row = lax.broadcasted_iota(jnp.int32, (8, C), 0)
    total = group_sum(jnp.where(row == 0, one, two))
    drift = total[0:1] * (1.0 / (sum(p.shape[0] for p in parts) * share))
    spread = jnp.maximum(total[1:2] - total[0:1] * drift, 0.0)
    store_stats(pivot + drift, spread, out_ref)


def affine(stats, gain, shift, rows):
    count = stats.shape[0]
    local = rows * (C // GROUPS)
    means = stats[:, 0:4, :]
    mean = jnp.sum(means, 0) * (1.0 / count)
    offset = means - mean[None]
    total = jnp.sum(stats[:, 4:8, :], 0) + local * jnp.sum(offset * offset, 0)
    inverse = lax.rsqrt(total * (1.0 / (local * count)) + EPS)
    flat = lambda v: jnp.concatenate([v[i : i + 1] for i in range(4)], axis=1)
    scale = flat(inverse) * gain
    return scale, shift - flat(mean) * scale


def pick(flags_ref, row, yes, no):
    flag = flags_ref[row : row + 1, :]
    wanted = jnp.broadcast_to(jnp.concatenate([flag] * (C // LANES), axis=1), yes.shape) > 0.0
    return jnp.where(wanted, yes, no)


def stats_kernel(x_ref, out_ref):
    half = x_ref.shape[0] // 2
    field_stats([x_ref[:half, :].astype(F32), x_ref[half:, :].astype(F32)], out_ref)


def fold_kernel(transposed, left_ref, right_ref, *refs):
    dims = (((1,), (1 if transposed else 0,)), ((), ()))
    product = lax.dot_general(left_ref[...], right_ref[...], dims, preferred_element_type=F32)
    refs[-1][...] = product.astype(BF16)


def fold(left, right, transposed, *early):
    def kernel(*refs):
        fold_kernel(transposed, *refs)

    args = [left, right, *early]
    out = jax.ShapeDtypeStruct((C, C), BF16)
    return call(kernel, out, [VMEM] * len(args), args, AHEAD, 8)


def query_kernel(
    flags_ref, x_ref, far_ref, stats_ref, gain_ref, shift_ref, wqk_ref, q_ref, coef_ref, halo_ref
):
    rows = x_ref.shape[0]
    scale, shift = affine(stats_ref[...], gain_ref[...], shift_ref[...], rows)
    coef_ref[0:1, :] = scale
    coef_ref[1:2, :] = shift
    halo = pick(flags_ref, 2, far_ref[rows - W : rows, :], far_ref[0:W, :])
    halo_ref[...] = halo
    for x, at in ((x_ref[...], slice(0, rows)), (halo, slice(rows, rows + W))):
        normed = (x.astype(F32) * scale + shift).astype(BF16)
        q = jnp.dot(normed, wqk_ref[...], preferred_element_type=F32)
        q_ref[at, :] = (q * (scale * (LOG2E / C**0.5))).astype(BF16)


BLOCK = 320
TILE = 256


def scores_of(q, keys):
    return [
        lax.dot_general(q, k[...], (((1,), (1,)), ((), ())), preferred_element_type=F32)
        for k in keys
    ]


def wide(v):
    return jnp.concatenate([v] * (C // LANES), axis=1)


def absorb(scores, keys, state):
    tiles = [t[:, j : j + LANES] for t in scores for j in range(0, t.shape[1], LANES)]
    top = tiles[0]
    for t in tiles[1:]:
        top = jnp.maximum(top, t)
    top = jnp.broadcast_to(jnp.max(top, axis=1, keepdims=True), top.shape)
    if state is not None:
        acc0, before, part0 = state
        top = jnp.maximum(before, top)
    part = None
    acc = None
    n = 0
    for t, k in zip(scores, keys):
        probs = []
        for _ in range(t.shape[1] // LANES):
            p = jnp.exp2(tiles[n] - top).astype(BF16)
            probs.append(p)
            p32 = p.astype(F32)
            part = p32 if part is None else part + p32
            n += 1
        d = jnp.dot(jnp.concatenate(probs, axis=1), k[...], preferred_element_type=F32)
        acc = d if acc is None else acc + d
    if state is not None:
        fade = jnp.exp2(before - top)
        part = part + part0 * fade
        acc = acc + acc0 * wide(fade)
    return acc, top, part


def pack(ref, at, acc, top, part):
    ref[at, 0:C] = acc
    total = jnp.broadcast_to(jnp.sum(part, axis=1, keepdims=True), top.shape)
    lane = lax.broadcasted_iota(jnp.int32, top.shape, 1)
    ref[at, C : C + LANES] = jnp.where(lane < LANES // 2, top, total)


def attend_kernel(n_q, n_k, first, packed, *refs):
    queries, keys, refs = refs[:n_q], refs[n_q : n_q + n_k], refs[n_q + n_k :]
    if not first:
        states, refs = [refs[3 * i : 3 * i + 3] for i in range(n_q)], refs[3 * n_q :]
    work = [
        (i, slice(at, at + BLOCK)) for i in range(n_q) for at in range(0, queries[i].shape[0], BLOCK)
    ]
    ahead = scores_of(queries[0][work[0][1], :], keys)
    for n, (i, at) in enumerate(work):
        now = ahead
        if n + 1 < len(work):
            j, to = work[n + 1]
            ahead = scores_of(queries[j][to, :], keys)
        state = None if first else tuple(r[at, :] for r in states[i])
        result = absorb(now, keys, state)
        if packed and i == 1:
            pack(refs[3], at, *result)
        else:
            for ref, v in zip(refs[3 * i : 3 * i + 3], result):
                ref[at, :] = v


def attend(queries, keys, state, packed=False):
    half = queries[0].shape[0]
    first = state is None
    n_q, n_k = len(queries), len(keys)
    one = [
        jax.ShapeDtypeStruct((half, C), F32),
        jax.ShapeDtypeStruct((half, LANES), F32),
        jax.ShapeDtypeStruct((half, LANES), F32),
    ]
    outs = one * n_q
    if packed:
        outs = one + [jax.ShapeDtypeStruct((half, C + LANES), F32)]
    args = [*queries, *keys] + ([] if first else list(state))
    aliases = {} if first else {n_q + n_k + i: i for i in range(3 if packed else 3 * n_q)}

    def kernel(*refs):
        attend_kernel(n_q, n_k, first, packed, *refs)

    flops = 4 * n_q * half * C * sum(k.shape[0] for k in keys)
    return call(kernel, outs, [VMEM] * len(args), args, flops, 20, aliases=aliases)


def output_kernel(
    flags_ref, q_ref, key_ref, acc_ref, top_ref, part_ref, met_ref, x_ref, halo_ref, coef_ref,
    wvo_ref, hidden_ref, stats_ref, inside_ref, outside_ref,
):
    keys = [key_ref]
    rows = x_ref.shape[0]
    half = rows // 2
    blocks = [slice(0, half), slice(half, rows), slice(rows, rows + W)]
    parts = []
    ahead = scores_of(q_ref[blocks[0], :], keys)
    for n, at in enumerate(blocks):
        now = ahead
        if n + 1 < len(blocks):
            ahead = scores_of(q_ref[blocks[n + 1], :], keys)
        acc, top, part = absorb(now, keys, (acc_ref[at, :], top_ref[at, :], part_ref[at, :]))
        total = jnp.broadcast_to(jnp.sum(part, axis=1, keepdims=True), top.shape)
        edge = met_ref[at, C : C + LANES]
        other = jnp.broadcast_to(edge[:, 0:1], top.shape)
        other_total = jnp.broadcast_to(edge[:, LANES - 1 : LANES], top.shape)
        most = jnp.maximum(top, other)
        wa, wb = jnp.exp2(top - most), jnp.exp2(other - most)
        inverse = 1.0 / (total * wa + other_total * wb)
        mixed = acc * wide(wa * inverse) + met_ref[at, 0:C] * wide(wb * inverse)
        normed = (mixed * coef_ref[0:1, :] + coef_ref[1:2, :]).astype(BF16)
        x = halo_ref[...] if at.start == rows else x_ref[at, :]
        hidden = x.astype(F32) + jnp.dot(normed, wvo_ref[...], preferred_element_type=F32)
        if at.start == rows:
            outside_ref[...] = hidden.astype(BF16)
        else:
            hidden_ref[at, :] = hidden.astype(BF16)
            parts.append(hidden.astype(BF16).astype(F32))
        if n == 1:
            field_stats(parts, stats_ref)
    inside_ref[...] = pick(
        flags_ref, 2, hidden_ref[rows - W : rows, :], hidden_ref[0:W, :]
    )


def conv_kernel(
    flags_ref, h_ref, inside_ref, outside_ref, stats_ref, gain_ref, shift_ref, w_ref, bias_ref,
    out_ref, left_ref, mid_ref, right_ref,
):
    rows = h_ref.shape[0]
    scale, shift = affine(stats_ref[...], gain_ref[...], shift_ref[...], rows)
    scale, shift = 0.5 * scale, 0.5 * shift

    def activate(f, at, keep):
        v = f.astype(F32) * scale + shift
        v = v + v * jnp.tanh(v)
        if keep is not None:
            v = pick(flags_ref, keep, v, jnp.zeros_like(v))
        column = lax.broadcasted_iota(jnp.int32, v.shape, 0) % W
        mid_ref[at : at + W, :] = v.astype(BF16)
        before = jnp.where(column == 0, 0.0, pltpu.roll(v, 1, 0))
        left_ref[at : at + W, :] = before.astype(BF16)
        after = jnp.where(column == W - 1, 0.0, pltpu.roll(v, W - 1, 0))
        right_ref[at : at + W, :] = after.astype(BF16)

    inside, outside = inside_ref[...].astype(F32), outside_ref[...].astype(F32)
    activate(pick(flags_ref, 2, outside, inside), 0, 0)
    for r in range(rows // W):
        activate(h_ref[r * W : (r + 1) * W, :], (r + 1) * W, None)
    activate(pick(flags_ref, 2, inside, outside), rows + W, 1)
    for r in range(0, rows, TILE):
        for n in range(0, C, TILE):
            total = None
            for dy in range(3):
                for dx, src in enumerate((left_ref, mid_ref, right_ref)):
                    d = jnp.dot(
                        src[r + dy * W : r + dy * W + TILE, :],
                        w_ref[3 * dy + dx, :, n : n + TILE],
                        preferred_element_type=F32,
                    )
                    total = d if total is None else total + d
            base = h_ref[r : r + TILE, n : n + TILE].astype(F32)
            out_ref[r : r + TILE, n : n + TILE] = (
                base + (total + bias_ref[:, n : n + TILE])
            ).astype(BF16)


def everyone(tile):
    count = lax.axis_size("row")
    copies = jnp.broadcast_to(tile, (count, *tile.shape))
    return lax.all_to_all(copies, "row", split_axis=0, concat_axis=0, tiled=True)


def local(
    latent, attn_gain, attn_shift, w_query, w_key, w_value, w_out,
    conv_gain, conv_shift, w_conv, conv_bias,
):
    count = lax.axis_size("row")
    chips = count // 2
    rows = latent.shape[0] * W
    me = lax.axis_index("row")
    place = lax.broadcasted_iota(jnp.int32, (8, LANES), 0)
    holds = [me > 0, me < count - 1, me % 2 == 0]
    flags = sum(jnp.where((place == i) & h, 1.0, 0.0) for i, h in enumerate(holds))
    latent, flags = lax.optimization_barrier((latent, flags))
    x = latent.reshape(rows, C)
    line = lambda v: v.reshape(1, C)
    swap = [(i, i ^ 1) for i in range(count)]
    ring = [(i, ((i // 2 + 1 - 2 * (i % 2)) % chips) * 2 + i % 2) for i in range(count)]

    move = lambda v, to: lax.ppermute(v, "row", to)
    tile = jax.ShapeDtypeStruct((8, LANES), F32)
    stats = call(stats_kernel, tile, [VMEM], [x], AHEAD)
    wqk = fold(w_query, w_key, True)
    taps = w_conv.reshape(9, C, C)
    wvo = fold(w_value, w_out, False, taps)
    near, far = x, move(x, swap)
    pieces = [x]
    for _ in range(1, chips // 2):
        near = move(near, ring)
        far = move(far, ring)
        pieces += [near, far]
    last_a = move(near[: rows // 2], ring)
    last_b = move(near[rows // 2 :], ring)

    stats = everyone(stats)
    query, coef, halo = call(
        query_kernel,
        [
            jax.ShapeDtypeStruct((rows + W, C), BF16),
            jax.ShapeDtypeStruct((8, C), F32),
            jax.ShapeDtypeStruct((W, C), BF16),
        ],
        [VMEM] * 7,
        [flags, x, pieces[2], stats, line(attn_gain), line(attn_shift), wqk],
        2 * rows * C * C,
    )
    other = move(query, swap)
    state = None
    for n, key in enumerate(pieces):
        state = attend([query, other], [key], state, n == len(pieces) - 1)
    *mine, theirs = state
    met = move(theirs, swap)
    across_a = move(last_a, swap)
    mine = attend([query], [last_a], mine)
    across = move(last_b, swap)
    mine = attend([query], [across_a, last_b], mine)
    edge = jax.ShapeDtypeStruct((W, C), BF16)
    hidden, tile2, inside, outside = call(
        output_kernel,
        [jax.ShapeDtypeStruct((rows, C), BF16), tile, edge, edge],
        [VMEM] * 11,
        [flags, query, across, *mine, met, x, halo, coef, wvo],
        6 * rows * C * C,
        20,
    )
    inside = move(inside, swap)
    stats2 = everyone(tile2)
    encoded = call(
        conv_kernel,
        jax.ShapeDtypeStruct((rows, C), BF16),
        [VMEM] * 9,
        [
            flags, hidden, inside, outside, stats2, line(conv_gain), line(conv_shift),
            taps, line(conv_bias),
        ],
        18 * rows * C * C,
        scratch=[pltpu.VMEM((rows + 2 * W, C), BF16)] * 3,
    )
    return encoded.reshape(latent.shape)


def solution(mesh):
    in_specs = (P(("img", "row"), None, None), P(), P(), P(), P(), P(), P(), P(), P(), P(), P())
    out_specs = P(("img", "row"), None, None)
    return jax.shard_map(local, mesh=mesh, in_specs=in_specs, out_specs=out_specs, check_vma=False)
```
